8 devices in a mesh: dp: 1 (over z), tp: 2 (over y), cp: 4 (over x, core).
Axes of the slice: x: 2, y: 2, z: 1, core: 2. Of those that a mesh axis runs over, the one named last changes fastest.
Arguments:
- x_in: bfloat16 [8192, 1536], P(('dp', 'cp', 'tp'))
- seg_ids: int32 [8192], P(('dp', 'cp', 'tp'))
- w_q: bfloat16 [1536, 12, 128], P(None, 'tp')
- w_k: bfloat16 [1536, 2, 128], P(None, 'tp')
- w_v: bfloat16 [1536, 2, 128], P(None, 'tp')
- w_o: bfloat16 [12, 128, 1536], P('tp')
Outputs:
- output: bfloat16 [8192, 1536], P(('dp', 'cp', 'tp'))
All inputs are finite; a program needn't handle non-finite values.
Results may differ from the reference program's by a relative error of at most 0.00413853.
Values are sent between devices in bfloat16 or wider.
A program may use at most 1 GiB of HBM per device.

```python
import jax
import jax.numpy as jnp
from jax import lax

CP = 4
PIECE = 1024
D = 1536
HEADS = 12
KV_HEADS = 2
HEAD = 128
DOCS = 6
QROWS = 64
SEQ = 2 * CP * PIECE
GROUP = HEADS // KV_HEADS


def row_positions():
    row_idx = jnp.arange(SEQ)
    owner_rank = row_idx // (2 * PIECE)
    within = row_idx % (2 * PIECE)
    return jnp.where(within < PIECE, owner_rank * PIECE + within, (2 * CP - 1 - owner_rank) * PIECE + within - PIECE)


def draw_segments(seg_key):
    half_len = SEQ // 2
    key_cut, key_gap = jax.random.split(seg_key)
    offsets = jax.random.permutation(key_cut, half_len - 1)[: DOCS - 1] + 1
    gap_start = jax.random.randint(key_gap, (), 0, half_len)
    cut_points = offsets + half_len * (offsets > gap_start).astype(jnp.int32)
    seq_pos = jnp.arange(SEQ)
    seg_seq = jnp.sum((seq_pos[:, None] >= cut_points[None, :]).astype(jnp.int32), axis=1)
    return seg_seq[row_positions()].astype(jnp.int32)


def setup_inputs(seed: int = 0, part: int = 0) -> dict:
    part_key = jax.random.fold_in(jax.random.key(seed), part)
    key_x, key_seg = jax.random.split(part_key)
    key_q, key_k, key_v, key_o = jax.random.split(jax.random.key(seed + 1), 4)
    x_in = jax.random.normal(key_x, (SEQ, D), jnp.float32).astype(jnp.bfloat16)
    seg_ids = draw_segments(key_seg)
    w_q = (jax.random.normal(key_q, (D, HEADS, HEAD), jnp.float32) * (1.5 * D ** -0.5)).astype(jnp.bfloat16)
    w_k = (jax.random.normal(key_k, (D, KV_HEADS, HEAD), jnp.float32) * D ** -0.5).astype(jnp.bfloat16)
    w_v = (jax.random.normal(key_v, (D, KV_HEADS, HEAD), jnp.float32) * D ** -0.5).astype(jnp.bfloat16)
    w_o = (jax.random.normal(key_o, (HEADS, HEAD, D), jnp.float32) * (4.0 * (HEADS * HEAD) ** -0.5)).astype(jnp.bfloat16)
    return {"x_in": x_in, "seg_ids": seg_ids, "w_q": w_q, "w_k": w_k, "w_v": w_v, "w_o": w_o}


def reference(x_in, seg_ids, w_q, w_k, w_v, w_o):
    pos_rows = row_positions()
    q_rows = jnp.dot(x_in, w_q.reshape(D, HEADS * HEAD), preferred_element_type=jnp.float32).astype(jnp.bfloat16)
    k_rows = jnp.dot(x_in, w_k.reshape(D, KV_HEADS * HEAD), preferred_element_type=jnp.float32).astype(jnp.bfloat16)
    v_rows = jnp.dot(x_in, w_v.reshape(D, KV_HEADS * HEAD), preferred_element_type=jnp.float32).astype(jnp.bfloat16)
    q_blocks = q_rows.reshape(SEQ // QROWS, QROWS, KV_HEADS, GROUP, HEAD).astype(jnp.float32)
    k_heads = k_rows.reshape(SEQ, KV_HEADS, HEAD).transpose(1, 0, 2).astype(jnp.float32)
    v_heads = v_rows.reshape(SEQ, KV_HEADS, HEAD).transpose(1, 0, 2).astype(jnp.float32)
    pos_blocks = pos_rows.reshape(SEQ // QROWS, QROWS)
    seg_blocks = seg_ids.reshape(SEQ // QROWS, QROWS)

    def query_block(blk_args):
        q_blk, pos_blk, seg_blk = blk_args
        visible = (seg_blk[:, None] == seg_ids[None, :]) & (pos_rows[None, :] <= pos_blk[:, None])

        def kv_head(head_args):
            q_head, k_head, v_head = head_args
            scores = jnp.einsum("qge,se->gqs", q_head, k_head) * HEAD ** -0.5
            scores = jnp.where(visible[None], scores, -jnp.inf)
            prob_rows = jnp.exp(scores - jnp.max(scores, axis=-1, keepdims=True))
            row_sum = jnp.sum(prob_rows, axis=-1)
            pv_sum = jnp.einsum("gqs,se->gqe", prob_rows.astype(jnp.bfloat16).astype(jnp.float32), v_head)
            return (pv_sum / row_sum[..., None]).astype(jnp.bfloat16)

        return lax.map(kv_head, (q_blk.transpose(1, 0, 2, 3), k_heads, v_heads))

    attn_rows = lax.map(query_block, (q_blocks, pos_blocks, seg_blocks))
    attn_rows = attn_rows.transpose(0, 3, 1, 2, 4).reshape(SEQ, HEADS * HEAD)
    y_out = jnp.dot(attn_rows, w_o.reshape(HEADS * HEAD, D), preferred_element_type=jnp.float32)
    return y_out.astype(jnp.bfloat16)
```

```python
import functools

import jax
import jax.numpy as jnp
import numpy as np
from jax import lax
from jax.experimental import pallas as pl
from jax.experimental.pallas import tpu as pltpu
from jax.sharding import PartitionSpec as P


NEG = -3e38
MIB = 1024 * 1024
BQ = 512
BK = 512
QC = 256
DEPTH = 3
VMEM = pltpu.VMEM
SMEM = pltpu.SMEM


def cost(us):
    return pl.CostEstimate(flops=int(us * 1e9), bytes_accessed=0, transcendentals=0)


def proj_kernel(n_x, with_kv, with_q, c_ref, *refs):
    refs = list(refs)
    x_refs = [refs.pop(0) for _ in range(n_x)]
    if with_kv:
        wk_ref, wv_ref = refs.pop(0), refs.pop(0)
    if with_q:
        wq_ref = refs.pop(0)
    if with_kv:
        kv_ref = refs.pop(0)
        x = x_refs[0][...]
        k = jnp.dot(x, wk_ref[...], preferred_element_type=jnp.float32)
        v = jnp.dot(x, wv_ref[...], preferred_element_type=jnp.float32)
        kv_ref[0] = k.astype(jnp.bfloat16)
        for j in range(x.shape[0] // 128):
            kv_ref[1, j * 128 : (j + 1) * 128, :] = v[j * 128 : (j + 1) * 128, :].T.astype(jnp.bfloat16)
    if with_q:
        for x_ref in x_refs:
            q_ref = refs.pop(0)
            x = x_ref[...]
            for g in range(wq_ref.shape[0]):
                q = jnp.dot(x, wq_ref[g], preferred_element_type=jnp.float32)
                q_ref[:, g * 128 : (g + 1) * 128] = q.astype(jnp.bfloat16)


def project(c_arr, xs, wkv, wq, heads, name):
    rows, width = xs[0].shape
    tile = 256
    in_specs = [pl.BlockSpec((tile, width), lambda i, c: (i, 0)) for _ in xs]
    args = list(xs)
    out_specs, out_shape = [], []
    if wkv is not None:
        in_specs += [pl.BlockSpec((width, 128), lambda i, c: (0, 0))] * 2
        args += list(wkv)
        out_specs.append(pl.BlockSpec((2, tile, 128), lambda i, c: (0, i, 0)))
        out_shape.append(jax.ShapeDtypeStruct((2, rows, 128), jnp.bfloat16))
    if wq is not None:
        if wq.shape[0] == heads:
            in_specs.append(pl.BlockSpec((heads, width, 128), lambda i, c: (0, 0, 0)))
        else:
            in_specs.append(pl.BlockSpec((heads, width, 128), lambda i, c: (c[0], 0, 0)))
        args.append(wq)
        for _ in xs:
            out_specs.append(pl.BlockSpec((tile, heads * 128), lambda i, c: (i, 0)))
            out_shape.append(jax.ShapeDtypeStruct((rows, heads * 128), jnp.bfloat16))
    return pl.pallas_call(
        functools.partial(proj_kernel, len(xs), wkv is not None, wq is not None),
        grid_spec=pltpu.PrefetchScalarGridSpec(
            num_scalar_prefetch=1, grid=(rows // tile,), in_specs=in_specs, out_specs=out_specs
        ),
        out_shape=out_shape,
        compiler_params=pltpu.CompilerParams(vmem_limit_bytes=40 * MIB),
        cost_estimate=cost(1.5 * len(xs)),
        name=name,
    )(c_arr, *args)


def table_kernel(n_cp, piece, docs, *refs):
    seg_refs, (tab_ref, qst_ref) = refs[:-2], refs[-2:]
    cp = lax.axis_index("cp")
    tp = lax.axis_index("tp")
    segs = [r[...] for r in seg_refs]
    starts = []
    for d in range(1, docs):
        n = jnp.zeros_like(segs[0])
        for s in segs:
            n = n + (s < d).astype(jnp.int32)
        starts.append(jnp.sum(n))
    for half, seg in enumerate(segs[:2]):
        st = jnp.zeros_like(seg)
        for d in range(1, docs):
            st = jnp.where(seg >= d, starts[d - 1], st)
        r = cp if half == 0 else cp ^ 1
        pos0 = jnp.where(tp == 0, r, 2 * n_cp - 1 - r) * piece
        rows = seg.shape[0]
        for i in range(rows):
            qst_ref[half, :, i * 128 : (i + 1) * 128] = st[i : i + 1, :]
        per = BQ // 128
        for b in range(rows // per):
            sub = st[b * per : (b + 1) * per, :]
            at = 8 + 4 * (half * (rows // per) + b)
            tab_ref[at] = pos0 + b * BQ
            tab_ref[at + 1] = jnp.min(sub)
            tab_ref[at + 2] = jnp.max(sub)
            tab_ref[at + 3] = 0
    tab_ref[0] = cp & 1
    tab_ref[1] = cp
    tab_ref[2] = tp
    for i in range(3, 8):
        tab_ref[i] = 0


def block_table(segs, n_cp, piece, docs):
    n_blocks = 2 * piece // BQ
    return pl.pallas_call(
        functools.partial(table_kernel, n_cp, piece, docs),
        in_specs=[pl.BlockSpec(memory_space=VMEM)] * len(segs),
        out_specs=[pl.BlockSpec(memory_space=SMEM), pl.BlockSpec(memory_space=VMEM)],
        out_shape=[
            jax.ShapeDtypeStruct((8 + 4 * n_blocks,), jnp.int32),
            jax.ShapeDtypeStruct((2, 1, piece), jnp.int32),
        ],
        cost_estimate=cost(1),
        name="block_table",
    )(*segs)


def attn_kernel(heads, n_cp, piece, other, state_in, state_out, tab, *refs):
    refs = list(refs)
    q_hbm = [refs.pop(0), refs.pop(0)]
    kv_hbm = [refs.pop(0) for _ in range(n_cp)]
    qst_ref = refs.pop(0)
    if state_in:
        acc_in, m_in, l_in = refs.pop(0), refs.pop(0), refs.pop(0)
    if state_out:
        acc_out, m_out, l_out = refs.pop(0), refs.pop(0), refs.pop(0)
    else:
        o_refs = [refs.pop(0), refs.pop(0)]
    q_s, kv_s, m_s, l_s, acc_s, s_s, p_s, a_s, sem = refs
    scale = float(np.log2(np.e) / np.sqrt(128.0))
    cp, tp = tab[1], tab[2]
    half = (1 - tp) if other else tp
    kbase = half * (n_cp * piece)
    copies = []
    for i in range(2):
        copies.append(pltpu.make_async_copy(q_hbm[i], q_s.at[i], sem.at[i]))
    for i in range(n_cp):
        r = cp ^ i
        slot = jnp.where(half == 0, r, n_cp - 1 - r)
        copies.append(pltpu.make_async_copy(kv_hbm[i], kv_s.at[slot], sem.at[2 + i]))
    for copy in copies:
        copy.start()
    for copy in copies:
        copy.wait()

    chunks = [(g, r) for g in range(heads) for r in range(0, BQ, QC)]
    n = len(chunks)
    n_kb = n_cp * piece // BK
    per = piece // BK
    per_q = piece // BQ

    def kblk(kb):
        return kv_s[kb // per, 0, pl.ds(pl.multiple_of((kb % per) * BK, BK), BK), :]

    def vblk(kb):
        off = pl.multiple_of((kb % per) * BK, BK)
        return jnp.concatenate([kv_s[kb // per, 1, pl.ds(off + j * 128, 128), :] for j in range(BK // 128)], axis=1)

    def q_block(b, _):
        qpos0, st_min, st_max = tab[8 + 4 * b], tab[9 + 4 * b], tab[10 + 4 * b]
        side = b // per_q
        q_off = pl.multiple_of((b % per_q) * BQ, BQ)
        end = n_cp * piece
        lo = jnp.clip(st_min - kbase, 0, end) // BK
        hi = (jnp.clip(qpos0 + BQ - kbase, 0, end) + BK - 1) // BK
        flo = (jnp.clip(st_max - kbase, 0, end) + BK - 1) // BK
        fhi = jnp.clip(qpos0 + 1 - kbase, 0, end) // BK
        if state_in:
            m_s[...] = m_in[b]
            l_s[...] = l_in[b]
            acc_s[...] = acc_in[b]
        else:
            m_s[...] = jnp.full_like(m_s, NEG)
            l_s[...] = jnp.zeros_like(l_s)
            acc_s[...] = jnp.zeros_like(acc_s)

        def qk(k, chunk):
            g, r = chunk
            q = q_s[side, pl.ds(q_off + r, QC), g * 128 : (g + 1) * 128]
            return lax.dot_general(k, q, (((1,), (1,)), ((), ())), preferred_element_type=jnp.float32)

        def fin(vt, chunk, p, a):
            g, r = chunk
            pv = jnp.dot(vt, p, preferred_element_type=jnp.float32)
            acc_s[g, :, r : r + QC] = a * acc_s[g, :, r : r + QC] + pv

        def step(kb, masked):
            k0 = kbase + kb * BK
            k, vt = kblk(kb), vblk(kb)
            k_next, v_prev = kblk(jnp.minimum(kb + 1, hi - 1)), vblk(jnp.maximum(kb - 1, lo))
            pend = None
            for ci, (g, r) in enumerate(chunks):
                s = s_s[ci % DEPTH]
                nx = ci + DEPTH
                s_new = qk(k, chunks[nx]) if nx < n else qk(k_next, chunks[nx - n])
                if pend is None:
                    fin(v_prev, chunks[-1], p_s[...], a_s[...])
                else:
                    fin(vt, *pend)
                if masked:
                    kpos = k0 + lax.broadcasted_iota(jnp.int32, (BK, QC), 0)
                    qpos = qpos0 + r + lax.broadcasted_iota(jnp.int32, (BK, QC), 1)
                    st = qst_ref[side, :, pl.ds(q_off + r, QC)]
                    s = jnp.where((kpos <= qpos) & (kpos >= st), s, NEG)
                m_old = m_s[g, :, r : r + QC]
                m_new = jnp.maximum(m_old, jnp.max(s, axis=0, keepdims=True))
                m_scaled = m_new * scale
                p = jnp.exp2(s * scale - m_scaled)
                a = jnp.exp2(m_old * scale - m_scaled)
                l_s[g, :, r : r + QC] = a * l_s[g, :, r : r + QC] + jnp.sum(p, axis=0, keepdims=True)
                m_s[g, :, r : r + QC] = m_new
                pend = ((g, r), p.astype(jnp.bfloat16), a)
                s_s[ci % DEPTH] = s_new
            p_s[...] = pend[1]
            a_s[...] = pend[2]

        @pl.when(hi > lo)
        def _():
            k = kblk(lo)
            for d in range(DEPTH):
                s_s[d] = qk(k, chunks[d])
            p_s[...] = jnp.zeros_like(p_s)
            a_s[...] = jnp.ones_like(a_s)

            def body(kb, carry):
                full = (kb >= flo) & (kb < fhi)

                @pl.when(full)
                def _():
                    step(kb, False)

                @pl.when(jnp.logical_not(full))
                def _():
                    step(kb, True)

                return carry

            lax.fori_loop(lo, hi, body, 0)
            fin(vblk(hi - 1), chunks[-1], p_s[...], a_s[...])

        if state_out:
            acc_out[b] = acc_s[...]
            m_out[b] = m_s[...]
            l_out[b] = l_s[...]
        else:
            for i in range(2):

                @pl.when(side == i)
                def _():
                    for g in range(heads):
                        o = (acc_s[g] / l_s[g]).T.astype(jnp.bfloat16)
                        o_refs[i][pl.ds(q_off, BQ), g * 128 : (g + 1) * 128] = o

        return 0

    lax.fori_loop(0, 2 * per_q, q_block, 0)


def attention(tab, qs, kvs, qst, state, last, other, n_cp, piece, us, name):
    heads = qs[0].shape[1] // 128
    n_blocks = 2 * piece // BQ
    any_spec = pl.BlockSpec(memory_space=pl.ANY)
    vmem_spec = pl.BlockSpec(memory_space=VMEM)
    state_shape = [
        jax.ShapeDtypeStruct((n_blocks, heads, 128, BQ), jnp.float32),
        jax.ShapeDtypeStruct((n_blocks, heads, 1, BQ), jnp.float32),
        jax.ShapeDtypeStruct((n_blocks, heads, 1, BQ), jnp.float32),
    ]
    args = [tab, *qs, *kvs, qst]
    in_specs = [pl.BlockSpec(memory_space=SMEM)] + [any_spec] * (2 + n_cp) + [vmem_spec]
    if state is not None:
        args += list(state)
        in_specs += [vmem_spec] * 3
    out_shape = [jax.ShapeDtypeStruct(qs[0].shape, jnp.bfloat16)] * 2 if last else state_shape
    return pl.pallas_call(
        functools.partial(attn_kernel, heads, n_cp, piece, other, state is not None, not last),
        in_specs=in_specs,
        out_specs=[vmem_spec] * len(out_shape),
        out_shape=out_shape,
        scratch_shapes=[
            VMEM((2, piece, heads * 128), jnp.bfloat16),
            VMEM((n_cp, 2, piece, 128), jnp.bfloat16),
            VMEM((heads, 1, BQ), jnp.float32),
            VMEM((heads, 1, BQ), jnp.float32),
            VMEM((heads, 128, BQ), jnp.float32),
            VMEM((DEPTH, BK, QC), jnp.float32),
            VMEM((BK, QC), jnp.bfloat16),
            VMEM((1, QC), jnp.float32),
            pltpu.SemaphoreType.DMA((2 + n_cp,)),
        ],
        compiler_params=pltpu.CompilerParams(vmem_limit_bytes=40 * MIB),
        cost_estimate=cost(us),
        name=name,
    )(*args)


def out_kernel(c_ref, *refs):
    o_refs, w_refs, y_ref = refs[:4], refs[4:8], refs[8]
    y = None
    for o_ref, w_ref in zip(o_refs, w_refs):
        w = w_ref[0] if len(w_ref.shape) == 3 else w_ref[...]
        part = jnp.dot(o_ref[...], w, preferred_element_type=jnp.float32)
        y = part if y is None else y + part
    y_ref[...] = y.astype(jnp.bfloat16)


def out_project(tab, outs, w_nat, w_for):
    rows, depth = outs[0].shape
    width = w_for[0].shape[1]
    tile = 256
    return pl.pallas_call(
        out_kernel,
        grid_spec=pltpu.PrefetchScalarGridSpec(
            num_scalar_prefetch=1,
            grid=(rows // tile,),
            in_specs=[pl.BlockSpec((tile, depth), lambda i, t: (i, 0))] * 4
            + [
                pl.BlockSpec((1, depth, width), lambda i, t: (t[0], 0, 0)),
                pl.BlockSpec((1, depth, width), lambda i, t: (1 - t[0], 0, 0)),
                pl.BlockSpec((depth, width), lambda i, t: (0, 0)),
                pl.BlockSpec((depth, width), lambda i, t: (0, 0)),
            ],
            out_specs=pl.BlockSpec((tile, width), lambda i, t: (i, 0)),
        ),
        out_shape=jax.ShapeDtypeStruct((rows, width), jnp.bfloat16),
        compiler_params=pltpu.CompilerParams(vmem_limit_bytes=40 * MIB),
        cost_estimate=cost(5),
        name="out_project",
    )(tab, *outs, w_nat, w_nat, *w_for)


def solution(mesh):
    n_cp = mesh.shape["cp"]
    n_tp = mesh.shape["tp"]
    docs = 6

    def core(a):
        return lax.ppermute(a, "cp", [(i, i ^ 1) for i in range(n_cp)])

    def across_x(a):
        return lax.ppermute(a, "cp", [(i, i ^ 2) for i in range(n_cp)])

    def across_y(a):
        return lax.ppermute(a, "tp", [(i, 1 - i) for i in range(n_tp)])

    def by_xor(a, k):
        return lax.ppermute(a, ("tp", "cp"), [(i, i ^ k) for i in range(n_tp * n_cp)])

    def per_device(x_loc, seg_loc, w_q, w_k, w_v, w_o):
        piece, width = x_loc.shape
        c = lax.axis_index("cp") & 1
        c_arr = jnp.full((1,), c, jnp.int32)
        heads = w_q.shape[1] // 2
        w_q = w_q.transpose(1, 0, 2)
        w_k = w_k.reshape(width, 128)
        w_v = w_v.reshape(width, 128)
        w_o = w_o.reshape(2, heads * 128, -1)

        seg = seg_loc.reshape(piece // 128, 128)
        segs = [seg] + [by_xor(seg, k) for k in range(1, n_tp * n_cp)]
        x_par = core(x_loc)
        wkv_one = across_y(jnp.where(c == 0, w_k, w_v))
        wkv_two = core(wkv_one)
        wk_f = jnp.where(c == 0, wkv_one, wkv_two)
        wv_f = jnp.where(c == 0, wkv_two, wkv_one)

        kv_n, q_n = project(c_arr, [x_loc], (w_k, w_v), w_q, heads, "proj_native")
        (q_n_par,) = project(c_arr, [x_par], None, w_q, heads, "proj_native_partner")
        (kv_f,) = project(c_arr, [x_loc], (wk_f, wv_f), None, heads, "proj_foreign_kv")
        tab, qst = block_table(segs, n_cp, piece, docs)

        def column(kv):
            far = across_x(kv)
            return [kv, core(kv), far, core(far)]

        same_n = column(kv_n)
        other_n = column(across_y(kv_f))
        same_f = column(kv_f)
        other_f = column(across_y(kv_n))
        wq_f = across_y(lax.dynamic_slice_in_dim(w_q, c * heads, heads, 0))
        wo_f = across_y(lax.dynamic_index_in_dim(w_o, c, 0, keepdims=False))
        wo_f_par = core(wo_f)

        att = functools.partial(attention, tab, n_cp=n_cp, piece=piece)
        q_nat = [q_n, q_n_par]
        st_n = att(q_nat, same_n, qst, None, False, False, us=18, name="attn_native_same")
        on_own, on_send = att(q_nat, other_n, qst, st_n, True, True, us=18, name="attn_native_other")
        on_par = core(on_send)
        q_for = project(c_arr, [x_loc, x_par], None, wq_f, heads, "proj_foreign_q")
        st_f = att(q_for, same_f, qst, None, False, False, us=18, name="attn_foreign_same")
        of_own, of_send = att(q_for, other_f, qst, st_f, True, True, us=18, name="attn_foreign_other")
        of_par = core(of_send)
        return out_project(tab, [on_own, on_par, of_own, of_par], w_o, [wo_f, wo_f_par])

    return jax.shard_map(
        per_device,
        mesh=mesh,
        in_specs=(P(("dp", "cp", "tp"), None), P(("dp", "cp", "tp")), P(None, "tp", None), P(None, "tp", None), P(None, "tp", None), P("tp", None, None)),
        out_specs=P(("dp", "cp", "tp"), None),
        check_vma=False,
    )
```

```python
import functools

import jax
import jax.numpy as jnp
import numpy as np
from jax import lax
from jax.experimental import pallas as pl
from jax.experimental.pallas import tpu as pltpu
from jax.sharding import PartitionSpec as P


NEG = -3e38
MIB = 1024 * 1024
BQ = 512
BK = 512
QC = 256
DEPTH = 3
VMEM = pltpu.VMEM
SMEM = pltpu.SMEM


def cost(us):
    return pl.CostEstimate(flops=int(us * 1e9), bytes_accessed=0, transcendentals=0)


def proj_kernel(n_x, with_kv, with_q, c_ref, *refs):
    refs = list(refs)
    x_refs = [refs.pop(0) for _ in range(n_x)]
    if with_kv:
        wk_ref, wv_ref = refs.pop(0), refs.pop(0)
    if with_q:
        wq_ref = refs.pop(0)
    if with_kv:
        kv_ref = refs.pop(0)
        x = x_refs[0][...]
        k = jnp.dot(x, wk_ref[...], preferred_element_type=jnp.float32)
        v = jnp.dot(x, wv_ref[...], preferred_element_type=jnp.float32)
        kv_ref[0] = k.astype(jnp.bfloat16)
        for j in range(x.shape[0] // 128):
            kv_ref[1, j * 128 : (j + 1) * 128, :] = v[j * 128 : (j + 1) * 128, :].T.astype(jnp.bfloat16)
    if with_q:
        for x_ref in x_refs:
            q_ref = refs.pop(0)
            x = x_ref[...]
            for g in range(wq_ref.shape[0]):
                q = jnp.dot(x, wq_ref[g], preferred_element_type=jnp.float32)
                q_ref[:, g * 128 : (g + 1) * 128] = q.astype(jnp.bfloat16)


def project(c_arr, xs, wkv, wq, heads, name):
    rows, width = xs[0].shape
    tile = 256
    in_specs = [pl.BlockSpec((tile, width), lambda i, c: (i, 0)) for _ in xs]
    args = list(xs)
    out_specs, out_shape = [], []
    if wkv is not None:
        in_specs += [pl.BlockSpec((width, 128), lambda i, c: (0, 0))] * 2
        args += list(wkv)
        out_specs.append(pl.BlockSpec((2, tile, 128), lambda i, c: (0, i, 0)))
        out_shape.append(jax.ShapeDtypeStruct((2, rows, 128), jnp.bfloat16))
    if wq is not None:
        if wq.shape[0] == heads:
            in_specs.append(pl.BlockSpec((heads, width, 128), lambda i, c: (0, 0, 0)))
        else:
            in_specs.append(pl.BlockSpec((heads, width, 128), lambda i, c: (c[0], 0, 0)))
        args.append(wq)
        for _ in xs:
            out_specs.append(pl.BlockSpec((tile, heads * 128), lambda i, c: (i, 0)))
            out_shape.append(jax.ShapeDtypeStruct((rows, heads * 128), jnp.bfloat16))
    return pl.pallas_call(
        functools.partial(proj_kernel, len(xs), wkv is not None, wq is not None),
        grid_spec=pltpu.PrefetchScalarGridSpec(
            num_scalar_prefetch=1, grid=(rows // tile,), in_specs=in_specs, out_specs=out_specs
        ),
        out_shape=out_shape,
        compiler_params=pltpu.CompilerParams(vmem_limit_bytes=63 * MIB),
        cost_estimate=cost(1.5 * len(xs)),
        name=name,
    )(c_arr, *args)


def table_kernel(n_cp, piece, docs, *refs):
    seg_refs, (tab_ref, qst_ref) = refs[:-2], refs[-2:]
    cp = lax.axis_index("cp")
    tp = lax.axis_index("tp")
    segs = [r[...] for r in seg_refs]
    starts = []
    for d in range(1, docs):
        n = jnp.zeros_like(segs[0])
        for s in segs:
            n = n + (s < d).astype(jnp.int32)
        starts.append(jnp.sum(n))
    for half, seg in enumerate(segs[:2]):
        st = jnp.zeros_like(seg)
        for d in range(1, docs):
            st = jnp.where(seg >= d, starts[d - 1], st)
        r = cp if half == 0 else cp ^ 1
        pos0 = jnp.where(tp == 0, r, 2 * n_cp - 1 - r) * piece
        rows = seg.shape[0]
        for i in range(rows):
            qst_ref[half, :, i * 128 : (i + 1) * 128] = st[i : i + 1, :]
        per = BQ // 128
        for b in range(rows // per):
            sub = st[b * per : (b + 1) * per, :]
            at = 8 + 4 * (half * (rows // per) + b)
            tab_ref[at] = pos0 + b * BQ
            tab_ref[at + 1] = jnp.min(sub)
            tab_ref[at + 2] = jnp.max(sub)
            tab_ref[at + 3] = 0
    tab_ref[0] = cp & 1
    tab_ref[1] = cp
    tab_ref[2] = tp
    for i in range(3, 8):
        tab_ref[i] = 0


def block_table(segs, n_cp, piece, docs):
    n_blocks = 2 * piece // BQ
    return pl.pallas_call(
        functools.partial(table_kernel, n_cp, piece, docs),
        in_specs=[pl.BlockSpec(memory_space=VMEM)] * len(segs),
        out_specs=[pl.BlockSpec(memory_space=SMEM), pl.BlockSpec(memory_space=VMEM)],
        out_shape=[
            jax.ShapeDtypeStruct((8 + 4 * n_blocks,), jnp.int32),
            jax.ShapeDtypeStruct((2, 1, piece), jnp.int32),
        ],
        cost_estimate=cost(1),
        name="block_table",
    )(*segs)


def attn_kernel(heads, n_cp, piece, other, state_in, state_out, tab, *refs):
    refs = list(refs)
    q_hbm = [refs.pop(0), refs.pop(0)]
    kv_hbm = [refs.pop(0) for _ in range(n_cp)]
    qst_ref = refs.pop(0)
    if state_in:
        acc_in, m_in, l_in = refs.pop(0), refs.pop(0), refs.pop(0)
    if state_out:
        acc_out, m_out, l_out = refs.pop(0), refs.pop(0), refs.pop(0)
    else:
        o_refs = [refs.pop(0), refs.pop(0)]
    q_s, kv_s, m_s, l_s, acc_s, s_s, p_s, a_s, sem = refs
    scale = float(np.log2(np.e) / np.sqrt(128.0))
    cp, tp = tab[1], tab[2]
    half = (1 - tp) if other else tp
    kbase = half * (n_cp * piece)
    copies = []
    for i in range(2):
        copies.append(pltpu.make_async_copy(q_hbm[i], q_s.at[i], sem.at[i]))
    for i in range(n_cp):
        r = cp ^ i
        slot = jnp.where(half == 0, r, n_cp - 1 - r)
        copies.append(pltpu.make_async_copy(kv_hbm[i], kv_s.at[slot], sem.at[2 + i]))
    for copy in copies:
        copy.start()
    for copy in copies:
        copy.wait()

    chunks = [(g, r) for g in range(heads) for r in range(0, BQ, QC)]
    n = len(chunks)
    n_kb = n_cp * piece // BK
    per = piece // BK
    per_q = piece // BQ

    def kblk(kb):
        return kv_s[kb // per, 0, pl.ds(pl.multiple_of((kb % per) * BK, BK), BK), :]

    def vblk(kb):
        off = pl.multiple_of((kb % per) * BK, BK)
        return jnp.concatenate([kv_s[kb // per, 1, pl.ds(off + j * 128, 128), :] for j in range(BK // 128)], axis=1)

    def q_block(b, _):
        qpos0, st_min, st_max = tab[8 + 4 * b], tab[9 + 4 * b], tab[10 + 4 * b]
        side = b // per_q
        q_off = pl.multiple_of((b % per_q) * BQ, BQ)
        end = n_cp * piece
        lo = jnp.clip(st_min - kbase, 0, end) // BK
        hi = (jnp.clip(qpos0 + BQ - kbase, 0, end) + BK - 1) // BK
        flo = (jnp.clip(st_max - kbase, 0, end) + BK - 1) // BK
        fhi = jnp.clip(qpos0 + 1 - kbase, 0, end) // BK
        if state_in:
            m_s[...] = m_in[b]
            l_s[...] = l_in[b]
            acc_s[...] = acc_in[b]
        else:
            m_s[...] = jnp.full_like(m_s, NEG)
            l_s[...] = jnp.zeros_like(l_s)
            acc_s[...] = jnp.zeros_like(acc_s)

        def qk(k, chunk):
            g, r = chunk
            q = q_s[side, pl.ds(q_off + r, QC), g * 128 : (g + 1) * 128]
            return lax.dot_general(k, q, (((1,), (1,)), ((), ())), preferred_element_type=jnp.float32)

        def fin(vt, chunk, p, a):
            g, r = chunk
            pv = jnp.dot(vt, p, preferred_element_type=jnp.float32)
            acc_s[g, :, r : r + QC] = a * acc_s[g, :, r : r + QC] + pv

        def step(kb, masked):
            k0 = kbase + kb * BK
            k, vt = kblk(kb), vblk(kb)
            k_next, v_prev = kblk(jnp.minimum(kb + 1, hi - 1)), vblk(jnp.maximum(kb - 1, lo))
            pend = None
            for ci, (g, r) in enumerate(chunks):
                s = s_s[ci % DEPTH]
                nx = ci + DEPTH
                s_new = qk(k, chunks[nx]) if nx < n else qk(k_next, chunks[nx - n])
                if pend is None:
                    fin(v_prev, chunks[-1], p_s[...], a_s[...])
                else:
                    fin(vt, *pend)
                if masked:
                    kpos = k0 + lax.broadcasted_iota(jnp.int32, (BK, QC), 0)
                    qpos = qpos0 + r + lax.broadcasted_iota(jnp.int32, (BK, QC), 1)
                    st = qst_ref[side, :, pl.ds(q_off + r, QC)]
                    s = jnp.where((kpos <= qpos) & (kpos >= st), s, NEG)
                m_old = m_s[g, :, r : r + QC]
                m_new = jnp.maximum(m_old, jnp.max(s, axis=0, keepdims=True))
                m_scaled = m_new * scale
                p = jnp.exp2(s * scale - m_scaled)
                a = jnp.exp2(m_old * scale - m_scaled)
                l_s[g, :, r : r + QC] = a * l_s[g, :, r : r + QC] + jnp.sum(p, axis=0, keepdims=True)
                m_s[g, :, r : r + QC] = m_new
                pend = ((g, r), p.astype(jnp.bfloat16), a)
                s_s[ci % DEPTH] = s_new
            p_s[...] = pend[1]
            a_s[...] = pend[2]

        @pl.when(hi > lo)
        def _():
            k = kblk(lo)
            for d in range(DEPTH):
                s_s[d] = qk(k, chunks[d])
            p_s[...] = jnp.zeros_like(p_s)
            a_s[...] = jnp.ones_like(a_s)

            def body(kb, carry):
                full = (kb >= flo) & (kb < fhi)

                @pl.when(full)
                def _():
                    step(kb, False)

                @pl.when(jnp.logical_not(full))
                def _():
                    step(kb, True)

                return carry

            lax.fori_loop(lo, hi, body, 0)
            fin(vblk(hi - 1), chunks[-1], p_s[...], a_s[...])

        if state_out:
            acc_out[b] = acc_s[...]
            m_out[b] = m_s[...]
            l_out[b] = l_s[...]
        else:
            for i in range(2):

                @pl.when(side == i)
                def _():
                    for g in range(heads):
                        o = (acc_s[g] / l_s[g]).T.astype(jnp.bfloat16)
                        o_refs[i][pl.ds(q_off, BQ), g * 128 : (g + 1) * 128] = o

        return 0

    lax.fori_loop(0, 2 * per_q, q_block, 0)


def attention(tab, qs, kvs, qst, state, last, other, n_cp, piece, us, name):
    heads = qs[0].shape[1] // 128
    n_blocks = 2 * piece // BQ
    any_spec = pl.BlockSpec(memory_space=pl.ANY)
    vmem_spec = pl.BlockSpec(memory_space=VMEM)
    state_shape = [
        jax.ShapeDtypeStruct((n_blocks, heads, 128, BQ), jnp.float32),
        jax.ShapeDtypeStruct((n_blocks, heads, 1, BQ), jnp.float32),
        jax.ShapeDtypeStruct((n_blocks, heads, 1, BQ), jnp.float32),
    ]
    args = [tab, *qs, *kvs, qst]
    in_specs = [pl.BlockSpec(memory_space=SMEM)] + [any_spec] * (2 + n_cp) + [vmem_spec]
    if state is not None:
        args += list(state)
        in_specs += [vmem_spec] * 3
    out_shape = [jax.ShapeDtypeStruct(qs[0].shape, jnp.bfloat16)] * 2 if last else state_shape
    return pl.pallas_call(
        functools.partial(attn_kernel, heads, n_cp, piece, other, state is not None, not last),
        in_specs=in_specs,
        out_specs=[vmem_spec] * len(out_shape),
        out_shape=out_shape,
        scratch_shapes=[
            VMEM((2, piece, heads * 128), jnp.bfloat16),
            VMEM((n_cp, 2, piece, 128), jnp.bfloat16),
            VMEM((heads, 1, BQ), jnp.float32),
            VMEM((heads, 1, BQ), jnp.float32),
            VMEM((heads, 128, BQ), jnp.float32),
            VMEM((DEPTH, BK, QC), jnp.float32),
            VMEM((BK, QC), jnp.bfloat16),
            VMEM((1, QC), jnp.float32),
            pltpu.SemaphoreType.DMA((2 + n_cp,)),
        ],
        compiler_params=pltpu.CompilerParams(vmem_limit_bytes=63 * MIB),
        cost_estimate=cost(us),
        name=name,
    )(*args)


def out_kernel(c_ref, *refs):
    o_refs, w_refs, y_ref = refs[:4], refs[4:8], refs[8]
    y = None
    for o_ref, w_ref in zip(o_refs, w_refs):
        w = w_ref[0] if len(w_ref.shape) == 3 else w_ref[...]
        part = jnp.dot(o_ref[...], w, preferred_element_type=jnp.float32)
        y = part if y is None else y + part
    y_ref[...] = y.astype(jnp.bfloat16)


def out_project(tab, outs, w_nat, w_for):
    rows, depth = outs[0].shape
    width = w_for[0].shape[1]
    tile = 256
    return pl.pallas_call(
        out_kernel,
        grid_spec=pltpu.PrefetchScalarGridSpec(
            num_scalar_prefetch=1,
            grid=(rows // tile,),
            in_specs=[pl.BlockSpec((tile, depth), lambda i, t: (i, 0))] * 4
            + [
                pl.BlockSpec((1, depth, width), lambda i, t: (t[0], 0, 0)),
                pl.BlockSpec((1, depth, width), lambda i, t: (1 - t[0], 0, 0)),
                pl.BlockSpec((depth, width), lambda i, t: (0, 0)),
                pl.BlockSpec((depth, width), lambda i, t: (0, 0)),
            ],
            out_specs=pl.BlockSpec((tile, width), lambda i, t: (i, 0)),
        ),
        out_shape=jax.ShapeDtypeStruct((rows, width), jnp.bfloat16),
        compiler_params=pltpu.CompilerParams(vmem_limit_bytes=63 * MIB),
        cost_estimate=cost(5),
        name="out_project",
    )(tab, *outs, w_nat, w_nat, *w_for)


def solution(mesh):
    n_cp = mesh.shape["cp"]
    n_tp = mesh.shape["tp"]
    docs = 6

    def core(a):
        return lax.ppermute(a, "cp", [(i, i ^ 1) for i in range(n_cp)])

    def across_x(a):
        return lax.ppermute(a, "cp", [(i, i ^ 2) for i in range(n_cp)])

    def across_y(a):
        return lax.ppermute(a, "tp", [(i, 1 - i) for i in range(n_tp)])

    def by_xor(a, k):
        return lax.ppermute(a, ("tp", "cp"), [(i, i ^ k) for i in range(n_tp * n_cp)])

    def per_device(x_loc, seg_loc, w_q, w_k, w_v, w_o):
        piece, width = x_loc.shape
        c = lax.axis_index("cp") & 1
        c_arr = jnp.full((1,), c, jnp.int32)
        heads = w_q.shape[1] // 2
        w_q = w_q.transpose(1, 0, 2)
        w_k = w_k.reshape(width, 128)
        w_v = w_v.reshape(width, 128)
        w_o = w_o.reshape(2, heads * 128, -1)

        seg = seg_loc.reshape(piece // 128, 128)
        segs = [seg] + [by_xor(seg, k) for k in range(1, n_tp * n_cp)]
        x_par = core(x_loc)
        wkv_one = across_y(jnp.where(c == 0, w_k, w_v))
        kv_n, q_n = project(c_arr, [x_loc], (w_k, w_v), w_q, heads, "proj_native")
        (q_n_par,) = project(c_arr, [x_par], None, w_q, heads, "proj_native_partner")
        tab, qst = block_table(segs, n_cp, piece, docs)
        wkv_two = core(wkv_one)
        wk_f = jnp.where(c == 0, wkv_one, wkv_two)
        wv_f = jnp.where(c == 0, wkv_two, wkv_one)
        (kv_f,) = project(c_arr, [x_loc], (wk_f, wv_f), None, heads, "proj_foreign_kv")

        att = functools.partial(attention, tab, n_cp=n_cp, piece=piece)
        near_n, far_n = core(kv_n), across_x(kv_n)
        same_n = [kv_n, near_n, far_n, core(far_n)]
        oth_n, diag_n = across_y(kv_f), by_xor(kv_f, n_cp + 2)
        st_n = att([q_n, q_n_par], same_n, qst, None, False, False, us=18, name="attn_native_same")
        oth_n, diag_n, wq_mine, kv_n2, kv_f2, st_n = lax.optimization_barrier(
            (oth_n, diag_n, lax.dynamic_slice_in_dim(w_q, c * heads, heads, 0), kv_n, kv_f, st_n)
        )
        other_n = [oth_n, core(oth_n), diag_n, core(diag_n)]
        wq_f = across_y(wq_mine)
        near_f, far_f = core(kv_f2), across_x(kv_f2)
        oth_f, diag_f = across_y(kv_n2), by_xor(kv_n2, n_cp + 2)
        on_own, on_send = att([q_n, q_n_par], other_n, qst, st_n, True, True, us=18, name="attn_native_other")
        far_f, wq_f, wo_mine, on_own, on_send = lax.optimization_barrier(
            (far_f, wq_f, lax.dynamic_index_in_dim(w_o, c, 0, keepdims=False), on_own, on_send)
        )
        on_par = core(on_send)
        wo_f = across_y(wo_mine)
        same_f = [kv_f, near_f, far_f, core(far_f)]
        q_for = project(c_arr, [x_loc, x_par], None, wq_f, heads, "proj_foreign_q")
        st_f = att(q_for, same_f, qst, None, False, False, us=18, name="attn_foreign_same")
        oth_f, diag_f, wo_f, on_par, st_f = lax.optimization_barrier((oth_f, diag_f, wo_f, on_par, st_f))
        other_f = [oth_f, core(oth_f), diag_f, core(diag_f)]
        wo_f_par = core(wo_f)
        of_own, of_send = att(q_for, other_f, qst, st_f, True, True, us=18, name="attn_foreign_other")
        of_par = core(of_send)
        return out_project(tab, [on_own, on_par, of_own, of_par], w_o, [wo_f, wo_f_par])

    return jax.shard_map(
        per_device,
        mesh=mesh,
        in_specs=(P(("dp", "cp", "tp"), None), P(("dp", "cp", "tp")), P(None, "tp", None), P(None, "tp", None), P(None, "tp", None), P("tp", None, None)),
        out_specs=P(("dp", "cp", "tp"), None),
        check_vma=False,
    )
```
